32 devices in a mesh: seq: 16 (over z, x, core), zero: 2 (over y).
Axes of the slice: x: 2, y: 2, z: 4, core: 2. Of those that a mesh axis runs over, the one named last changes fastest.
Arguments:
- tokens: bfloat16 [2, 2048, 2048], P('zero', 'seq'), may hold values from -6 to 6
- w_in: bfloat16 [2048, 2336], P('zero'), may hold values from -0.0625 to 0.0625
- a_log: float32 [32], replicated, may hold values from -8 to 0
- dt_bias: float32 [32], replicated, may hold values from -4.5 to -3.5
- d_skip: float32 [32], replicated, may hold values from 0.5 to 1.5
- grad_y: bfloat16 [2, 2048, 2048], P('zero', 'seq'), may hold values from -6 to 6
Outputs:
- y_out: bfloat16 [2, 2048, 2048], P('zero', 'seq')
- grad_tokens: bfloat16 [2, 2048, 2048], P('zero', 'seq')
- grad_w: float32 [2048, 2336], P(('seq', 'zero'))
The draws below stay inside these ranges and needn't reach their ends.
All inputs are finite; a program needn't handle non-finite values.
Results may differ from the reference program's by a relative error of at most 0.013.
Values may be sent and summed in bfloat16 or wider, within the bound.
No kernel may reach another device: no remote copies, remote signals or barrier semaphores. Data moves between devices by JAX's collectives and lax.ppermute only.
A program may use at most 128 MiB of HBM per device.

```python
import jax
import jax.numpy as jnp
from jax import lax

D = 2048
STATE = 128
HEADS = 32
HEAD_SIZE = 64
TOK_DEV = 128
INNER = 2048
PROJ = 2336
BATCH = 2
LENGTH = 2048
N_SEQ = 16


def block_scale(own_key, extent, shards, least, top_value):
    level, own = 1.0, jax.random.fold_in(own_key, 6)
    for axis_at, shards_of in shards:
        draws = jnp.exp(jax.random.uniform(jax.random.fold_in(own, axis_at), (shards_of,), jnp.float32, least / len(shards), top_value / len(shards)))
        level = level * jnp.repeat(draws, extent[axis_at] // shards_of).reshape([-1 if axis == axis_at else 1 for axis in range(len(extent))])
    return level


def noise(own_key, shape, scale, reach, cuts=(), kind=jnp.bfloat16):
    gain = block_scale(own_key, shape, cuts, -0.22, 0.18) if cuts else 1.0
    result = jax.random.normal(own_key, shape, jnp.float32) * scale * gain
    return jnp.minimum(jnp.maximum(result, -reach), reach).astype(kind)


def setup_inputs(seed: int = 0) -> dict:
    keys = jax.random.split(jax.random.key(seed), 7)
    return {
        "tokens": noise(keys[0], (BATCH, LENGTH, D), 1.0, 6.0, ((0, 2), (1, 16))),
        "w_in": noise(keys[1], (D, PROJ), (4 * D) ** -0.5, 0.0625, ((0, 2),)),
        "a_log": jnp.clip(jax.random.uniform(keys[2], (HEADS,), jnp.float32, -8.0, 0.0), -8.0, 0.0),
        "dt_bias": jnp.clip(jax.random.uniform(keys[3], (HEADS,), jnp.float32, -4.5, -3.5), -4.5, -3.5),
        "d_skip": jnp.clip(jax.random.uniform(keys[4], (HEADS,), jnp.float32, 0.5, 1.5), 0.5, 1.5),
        "grad_y": noise(keys[5], (BATCH, LENGTH, INNER), 1.0, 6.0, ((0, 2), (1, 16))),
    }


def block_ssd(xs, bm, cm, raw, start, a_log, dt_bias, d_skip):
    high = lax.Precision.HIGHEST
    dt = jax.nn.softplus(raw + dt_bias)
    loga = -jnp.exp(a_log) * dt
    cum = jnp.cumsum(loga, axis=0)
    count = xs.shape[0]
    later = (jnp.arange(count)[:, None] >= jnp.arange(count)[None, :])[:, :, None]
    spans = cum[:, None, :] - cum[None, :, :]
    decay = jnp.where(later, jnp.exp(jnp.where(later, spans, 0.0)), 0.0)
    scores = jnp.dot(cm, bm.T, precision=high)
    mixing = scores[:, :, None] * decay * dt[None, :, :]
    ssd = jnp.einsum('tsh,shp->thp', mixing, xs, precision=high)
    ssd = ssd + jnp.einsum('tn,th,hpn->thp', cm, jnp.exp(cum), start, precision=high)
    out = ssd + d_skip[None, :, None] * xs
    tail = jnp.exp(cum[-1:] - cum) * dt
    state = jnp.exp(cum[-1])[:, None, None] * start + jnp.einsum('sh,sn,shp->hpn', tail, bm, xs, precision=high)
    return (out, state)

def reference(tokens, w_in, a_log, dt_bias, d_skip, grad_y):
    proj = jnp.dot(tokens.reshape(BATCH * LENGTH, D), w_in, preferred_element_type=jnp.float32)
    proj = proj.reshape(BATCH, LENGTH, PROJ)
    xs = lax.optimization_barrier(proj[:, :, :INNER].astype(jnp.bfloat16)).astype(jnp.float32)
    bm = lax.optimization_barrier(proj[:, :, INNER:INNER + STATE].astype(jnp.bfloat16)).astype(jnp.float32)
    cm = lax.optimization_barrier(proj[:, :, INNER + STATE:INNER + 2 * STATE].astype(jnp.bfloat16)).astype(jnp.float32)
    raw = proj[:, :, INNER + 2 * STATE:]
    blocks = LENGTH // TOK_DEV

    def forward(xseq, bseq, cseq, rseq):
        xb = xseq.reshape(blocks, TOK_DEV, HEADS, HEAD_SIZE)
        bb = bseq.reshape(blocks, TOK_DEV, STATE)
        cb = cseq.reshape(blocks, TOK_DEV, STATE)
        rb = rseq.reshape(blocks, TOK_DEV, HEADS)

        def step(carry, item):
            out, state = block_ssd(item[0], item[1], item[2], item[3], carry, a_log, dt_bias, d_skip)
            return (state, out)
        initial = jnp.zeros((HEADS, HEAD_SIZE, STATE), jnp.float32)
        final, outs = lax.scan(step, initial, (xb, bb, cb, rb))
        return outs.reshape(LENGTH, INNER)

    def one_sequence(item):
        xseq, bseq, cseq, rseq, gseq = item
        out, pullback = jax.vjp(forward, xseq, bseq, cseq, rseq)
        gx, gb, gc, gr = pullback(gseq.astype(jnp.float32))
        return (out, jnp.concatenate([gx, gb, gc, gr], axis=1))
    outs, grads = lax.map(one_sequence, (xs, bm, cm, raw, grad_y))
    y_out = outs.astype(jnp.bfloat16)
    gproj = grads.astype(jnp.bfloat16)
    grad_tokens = jnp.dot(gproj.reshape(BATCH * LENGTH, PROJ), w_in.T, preferred_element_type=jnp.float32)
    grad_tokens = grad_tokens.astype(jnp.bfloat16).reshape(BATCH, LENGTH, D)
    ublocks = tokens.reshape(BATCH * N_SEQ, TOK_DEV, D)
    gblocks = gproj.reshape(BATCH * N_SEQ, TOK_DEV, PROJ)

    def add_part(total, item):
        part = jnp.dot(item[0].T, item[1], preferred_element_type=jnp.float32)
        part = lax.optimization_barrier(part.astype(jnp.bfloat16)).astype(jnp.float32)
        return (total + part, None)
    grad_w, unused = lax.scan(add_part, jnp.zeros((D, PROJ), jnp.float32), (ublocks, gblocks))
    return (y_out, grad_tokens, grad_w)
```

```python
import functools

import jax
import jax.numpy as jnp
from jax import lax
from jax.experimental import pallas as pl
from jax.experimental.pallas import tpu as pltpu
from jax.sharding import PartitionSpec as P

F32 = jnp.float32
BF16 = jnp.bfloat16
HIGH = lax.Precision.HIGHEST
LANES = 128


def dot(a, b, dims, precision=None):
    return lax.dot_general(
        a, b, ((dims[:1], dims[1:]), ((), ())), precision=precision, preferred_element_type=F32
    )


def triangles(count):
    row = lax.broadcasted_iota(jnp.int32, (count, count), 0)
    col = lax.broadcasted_iota(jnp.int32, (count, count), 1)
    return row, col


def spread(values, first, per, width):
    lane = lax.broadcasted_iota(jnp.int32, (values.shape[0], LANES), 1)
    out = values[:, first : first + 1]
    for k in range(1, per):
        out = jnp.where(lane < k * width, out, values[:, first + k : first + k + 1])
    return jnp.broadcast_to(out, (values.shape[0], LANES))


def head_lanes(tile, k, width):
    lane = lax.broadcasted_iota(jnp.int32, tile.shape, 1)
    keep = (lane >= k * width) & (lane < (k + 1) * width)
    return jnp.where(keep, tile, jnp.zeros_like(tile))


def prepare(inner, state, heads, n_back, own_ref, *refs):
    back_refs, refs = refs[:n_back], refs[n_back:]
    bias_ref, alog_ref, g_ref, xbc_ref, raw_ref, dt_ref, cum_ref, fb_ref, dec_ref = refs
    width = inner // heads
    per = LANES // width
    count = own_ref.shape[0]
    main = inner + 2 * state
    raw = own_ref[:, main : main + heads]
    for ref in back_refs:
        raw = raw + ref[:, main : main + heads].astype(F32)
        raw = raw + ref[:, main + heads : main + 2 * heads].astype(F32)
    shifted = raw + bias_ref[...]
    dt = jnp.maximum(shifted, 0.0) + jnp.log1p(jnp.exp(-jnp.abs(shifted)))
    loga = -jnp.exp(alog_ref[...]) * dt
    row, col = triangles(count)
    lower = (row >= col).astype(F32)
    cum = dot(lower, loga, (1, 0), HIGH)
    raw_ref[...] = raw
    dt_ref[...] = dt
    cum_ref[...] = cum
    total = cum[count - 1 : count, :]
    tail = jnp.exp(total - cum) * dt
    grow = jnp.exp(cum)
    onehot = (
        lax.broadcasted_iota(jnp.int32, (heads, heads), 0)
        == lax.broadcasted_iota(jnp.int32, (heads, heads), 1)
    ).astype(F32)
    decays = jnp.broadcast_to(jnp.exp(total), (LANES, heads))
    dec_ref[...] = dot(onehot, decays, (1, 1), HIGH)

    def column(at):
        part = own_ref[:, at : at + LANES]
        for ref in back_refs:
            part = part + ref[:, at : at + LANES].astype(F32)
        return part.astype(BF16)

    for at in range(inner, main, LANES):
        xbc_ref[:, at : at + LANES] = column(at)
    bm = xbc_ref[:, inner : inner + state]
    cm = xbc_ref[:, inner + state : main]
    for j in range(heads // per):
        at = j * LANES
        x = column(at)
        xbc_ref[:, at : at + LANES] = x
        scaled = (spread(tail, j * per, per, width) * x.astype(F32)).astype(BF16)
        fb_ref[0, at : at + LANES, :] = dot(scaled, bm, (0, 0)).astype(BF16)
        g = g_ref[:, at : at + LANES].astype(F32)
        grown = (spread(grow, j * per, per, width) * g).astype(BF16)
        fb_ref[1, at : at + LANES, :] = dot(grown, cm, (0, 0)).astype(BF16)


def within(inner, state, heads, xbc_ref, g_ref, dt_ref, cum_ref, y_ref, v_ref, w_ref):
    width = inner // heads
    per = LANES // width
    count = dt_ref.shape[0]
    main = inner + 2 * state
    bm = xbc_ref[:, inner : inner + state]
    cm = xbc_ref[:, inner + state : main]
    dt = dt_ref[...]
    cum = cum_ref[...]
    row, col = triangles(count)
    eye = (row == col).astype(F32)
    cum_rows = dot(cum, eye, (0, 0), HIGH)
    dt_rows = dot(dt, eye, (0, 0), HIGH)
    later = row >= col
    scores = dot(cm, bm, (1, 1))
    mixed = jnp.zeros((count, count), F32)
    for j in range(heads // per):
        at = j * LANES
        x = xbc_ref[:, at : at + LANES]
        g = g_ref[:, at : at + LANES]
        xdt = (spread(dt, j * per, per, width) * x.astype(F32)).astype(BF16)
        y = jnp.zeros((count, LANES), F32)
        v = jnp.zeros((count, LANES), F32)
        for k in range(per):
            h = j * per + k
            span = jnp.where(later, cum[:, h : h + 1] - cum_rows[h : h + 1, :], -1e30)
            decay = jnp.exp(span)
            weights = (scores * decay).astype(BF16)
            gk = head_lanes(g, k, width)
            mixed = mixed + decay * dt_rows[h : h + 1, :] * dot(gk, x, (1, 1))
            y = y + dot(weights, head_lanes(xdt, k, width), (1, 0))
            v = v + dot(weights, gk, (0, 0))
        y_ref[:, at : at + LANES] = y
        v_ref[:, at : at + LANES] = v
    w_ref[...] = mixed


def across(
    inner, state, heads, xbc_ref, g_ref, raw_ref, dt_ref, cum_ref, bias_ref, alog_ref, skip_ref,
    y_ref, v_ref, w_ref, se_ref, out_ref, gp_ref
):
    width = inner // heads
    per = LANES // width
    count = dt_ref.shape[0]
    main = inner + 2 * state
    bm = xbc_ref[:, inner : inner + state]
    cm = xbc_ref[:, inner + state : main]
    dt = dt_ref[...]
    cum = cum_ref[...]
    total = cum[count - 1 : count, :]
    grow = jnp.exp(cum)
    tail = jnp.exp(total - cum)
    skip = jnp.broadcast_to(skip_ref[...], (8, heads))
    mixed = w_ref[...].astype(BF16)
    grad_b = dot(mixed, cm, (0, 0))
    grad_c = dot(mixed, bm, (1, 0))
    head = lax.broadcasted_iota(jnp.int32, (count, heads), 1)
    head8 = lax.broadcasted_iota(jnp.int32, (8, heads), 1)
    near = jnp.zeros((count, heads), F32)
    far = jnp.zeros((count, heads), F32)
    direct = jnp.zeros((count, heads), F32)
    inside = jnp.zeros((8, heads), F32)
    for j in range(heads // per):
        at = j * LANES
        x16 = xbc_ref[:, at : at + LANES]
        x = x16.astype(F32)
        g = g_ref[:, at : at + LANES].astype(F32)
        start = se_ref[0, at : at + LANES, :]
        end = se_ref[1, at : at + LANES, :]
        dts = spread(dt, j * per, per, width)
        grows = spread(grow, j * per, per, width)
        tails = spread(tail, j * per, per, width)
        skips = spread(skip, j * per, per, width)[0:1, :]
        y = y_ref[:, at : at + LANES] + grows * dot(cm, start, (1, 1))
        v_in = v_ref[:, at : at + LANES]
        v_out = tails * dot(bm, end, (1, 1))
        v = v_in + v_out
        out_ref[:, at : at + LANES] = (y + skips * x).astype(BF16)
        gp_ref[:, at : at + LANES] = (dts * v + skips * g).astype(BF16)
        xdt = dts * x
        grad_b = grad_b + dot((tails * xdt).astype(BF16), end, (1, 0))
        grad_c = grad_c + dot((grows * g).astype(BF16), start, (1, 0))
        a = g * y - xdt.astype(BF16).astype(F32) * v_in
        q = xdt * v_out
        d = x * v
        es = end.astype(F32) * start.astype(F32)
        for k in range(per):
            h = j * per + k
            near = jnp.where(head == h, jnp.sum(head_lanes(a, k, width), 1, keepdims=True), near)
            far = jnp.where(head == h, jnp.sum(head_lanes(q, k, width), 1, keepdims=True), far)
            direct = jnp.where(head == h, jnp.sum(head_lanes(d, k, width), 1, keepdims=True), direct)
            rows = jnp.sum(es[k * width : (k + 1) * width, :], axis=0, keepdims=True)
            value = jnp.sum(rows, axis=1, keepdims=True)
            inside = jnp.where(head8 == h, value, inside)
    row, col = triangles(count)
    upper = (row <= col).astype(F32)
    before = (row > col).astype(F32)
    dloga = dot(upper, near, (1, 0), HIGH) + dot(before, far, (1, 0), HIGH)
    dloga = dloga + jnp.exp(total) * inside[0:1, :]
    slope = jax.nn.sigmoid(raw_ref[...] + bias_ref[...])
    grad_raw = slope * (direct - jnp.exp(alog_ref[...]) * dloga)
    gp_ref[:, inner : inner + state] = grad_b.astype(BF16)
    gp_ref[:, inner + state : main] = grad_c.astype(BF16)
    gp_ref[:, main : main + heads] = grad_raw.astype(BF16)


def local_call(body, outs, flops, name, *args):
    size = sum(a.size * a.dtype.itemsize for a in args)
    return pl.pallas_call(
        body,
        out_shape=outs,
        in_specs=[pl.BlockSpec(memory_space=pltpu.VMEM)] * len(args),
        out_specs=jax.tree.map(lambda _: pl.BlockSpec(memory_space=pltpu.VMEM), outs),
        cost_estimate=pl.CostEstimate(flops=flops, bytes_accessed=size, transcendentals=0),
        compiler_params=pltpu.CompilerParams(vmem_limit_bytes=40 * 2**20),
        name=name,
    )(*args)


def take(parts, at):
    return lax.dynamic_index_in_dim(parts, at, 0, keepdims=False)


def shifted_pairs(total, factor, stride, by):
    pairs = []
    for i in range(total):
        at = (i // stride) % factor
        pairs.append((i, i + ((at + by) % factor - at) * stride))
    return pairs


def deal(parts, axis, factor, stride):
    total = lax.axis_size(axis)
    me = (lax.axis_index(axis) // stride) % factor
    got = [take(parts, me)]
    for by in range(1, factor):
        piece = take(parts, (me + by) % factor)
        got.append(lax.ppermute(piece, axis, shifted_pairs(total, factor, stride, by)))
    return got


def in_order(got, axis, factor, stride):
    me = (lax.axis_index(axis) // stride) % factor
    if factor == 2:
        first = me == 0
        return [jnp.where(first, got[0], got[1]), jnp.where(first, got[1], got[0])]
    stacked = jnp.stack(got)
    return [take(stacked, (me - i) % factor) for i in range(factor)]


def exchange(parts, factor, stride):
    return in_order(deal(parts, "seq", factor, stride), "seq", factor, stride)


def carried(pair, decay, levels):
    (factor, stride), rest = levels[0], levels[1:]
    heads, width, state = pair.shape[1:]
    share = heads // factor
    parts = pair.reshape(2, factor, share, width, state).swapaxes(0, 1)
    got = [p.astype(F32) for p in exchange(parts, factor, stride)]
    dec = exchange(decay.reshape(factor, share, LANES), factor, stride)
    mul = [d[:, None, :state] for d in dec]
    if rest:
        ahead, behind, product = got[0][0], got[-1][1], dec[0]
        for i in range(1, factor):
            ahead = mul[i] * ahead + got[i][0]
            product = product * dec[i]
        for i in range(factor - 2, -1, -1):
            behind = mul[i] * behind + got[i][1]
        node = carried(jnp.stack([ahead, behind]).astype(BF16), product, rest).astype(F32)
        start, end = node[0], node[1]
    else:
        start = end = jnp.zeros((share, width, state), F32)
    starts, ends = [start], [end]
    for i in range(factor - 1):
        starts.append(mul[i] * starts[-1] + got[i][0])
    for i in range(factor - 1, 0, -1):
        ends.append(mul[i] * ends[-1] + got[i][1])
    ends = ends[::-1]
    send = jnp.stack([jnp.stack([s, e]) for s, e in zip(starts, ends)]).astype(BF16)
    return jnp.concatenate(exchange(send, factor, stride), axis=1)


def per_device(tokens, w_in, a_log, dt_bias, d_skip, grad_y):
    count, width = tokens.shape[1:]
    inner = grad_y.shape[2]
    heads = a_log.shape[0]
    columns = w_in.shape[1]
    state = (columns - inner - heads) // 2
    main = inner + 2 * state
    seq_count = lax.axis_size("seq")
    zero_count = lax.axis_size("zero")
    depth = w_in.shape[0]
    piece = width // (seq_count * zero_count)
    core = 2 if seq_count % 2 == 0 else 1
    mid = 2 if (seq_count // core) % 2 == 0 else 1
    outer = seq_count // (core * mid)
    rows = tokens.reshape(count, width)
    g = grad_y.reshape(count, inner)
    bias = dt_bias.reshape(1, heads)
    alog = a_log.reshape(1, heads)
    skip = d_skip.reshape(1, heads)

    slices = rows.reshape(count, zero_count, depth).swapaxes(0, 1)
    mine = deal(slices, "zero", zero_count, 1)
    backs = []
    for by in range(1, zero_count):
        part = jnp.dot(mine[by], w_in, preferred_element_type=F32)
        raw = part[:, main:]
        high = lax.reduce_precision(raw, 8, 7)
        sent = jnp.concatenate(
            [part[:, :main].astype(BF16), high.astype(BF16), (raw - high).astype(BF16)], axis=1
        )
        backs.append(
            lax.ppermute(sent, "zero", shifted_pairs(zero_count, zero_count, 1, -by))
        )
    own = jnp.dot(mine[0], w_in, preferred_element_type=F32)

    small = jax.ShapeDtypeStruct((count, heads), F32)
    xbc, raw, dt, cum, pair, decay = local_call(
        functools.partial(prepare, inner, state, heads, len(backs)),
        (
            jax.ShapeDtypeStruct((count, main), BF16),
            small,
            small,
            small,
            jax.ShapeDtypeStruct((2, inner, state), BF16),
            jax.ShapeDtypeStruct((heads, LANES), F32),
        ),
        4 * count * inner * state,
        "prepare",
        own, *backs, bias, alog, g,
    )
    wide = jax.ShapeDtypeStruct((count, inner), F32)
    y_near, v_near, mixed = local_call(
        functools.partial(within, inner, state, heads),
        (wide, wide, jax.ShapeDtypeStruct((count, count), F32)),
        20 * count * inner * count,
        "within",
        xbc, g, dt, cum,
    )
    levels = [lv for lv in ((core, 1), (mid, core), (outer, core * mid)) if lv[0] > 1]
    start_end = carried(pair.reshape(2, heads, inner // heads, state), decay, levels)
    y, gproj = local_call(
        functools.partial(across, inner, state, heads),
        (
            jax.ShapeDtypeStruct((count, inner), BF16),
            jax.ShapeDtypeStruct((count, columns), BF16),
        ),
        8 * count * inner * state,
        "across",
        xbc, g, raw, dt, cum, bias, alog, skip, y_near, v_near, mixed,
        start_end.reshape(2, inner, state),
    )

    by_owner = rows.reshape(count, outer, mid, core, zero_count, piece).transpose(4, 0, 3, 1, 2, 5)
    by_owner = by_owner.reshape(zero_count, count, core, outer * mid * piece)
    theirs = jnp.stack(deal(by_owner, "zero", zero_count, 1))
    theirs = theirs.transpose(2, 0, 1, 3).reshape(core, zero_count * count, outer * mid * piece)
    left = jnp.concatenate(deal(theirs, "seq", core, 1), axis=0)

    cotangents = [gproj] + [
        lax.ppermute(gproj, "zero", shifted_pairs(zero_count, zero_count, 1, by))
        for by in range(1, zero_count)
    ]
    grads = [
        lax.dot_general(c, w_in, (((1,), (1,)), ((), ())), preferred_element_type=F32).astype(BF16)
        for c in cotangents
    ]
    blocks = [grads[0]] + [
        lax.ppermute(grads[by], "zero", shifted_pairs(zero_count, zero_count, 1, -by))
        for by in range(1, zero_count)
    ]
    mine_at = lax.axis_index("zero")
    if zero_count == 2:
        ordered = in_order(blocks, "zero", zero_count, 1)
    else:
        stacked = jnp.stack(blocks)
        ordered = [take(stacked, (i - mine_at) % zero_count) for i in range(zero_count)]
    grad_tokens = jnp.concatenate(ordered, axis=1).reshape(1, count, width)

    both = jnp.concatenate(cotangents, axis=0)
    right = [both] + [
        lax.ppermute(both, "seq", shifted_pairs(seq_count, core, 1, by)) for by in range(1, core)
    ]
    right = jnp.concatenate(right, axis=0)
    grad = lax.dot_general(left, right, (((0,), (0,)), ((), ())), preferred_element_type=F32)
    for factor, stride in ((outer, core * mid), (mid, core)):
        parts = grad.astype(BF16).reshape(factor, grad.shape[0] // factor, columns)
        got = deal(parts, "seq", factor, stride)
        grad = sum(p.astype(F32) for p in got)
    return (y.reshape(1, count, inner), grad_tokens, grad)


def solution(mesh):
    placed = (P("zero", "seq", None), P("zero", None), P(), P(), P(), P("zero", "seq", None))
    return jax.shard_map(
        per_device,
        mesh=mesh,
        in_specs=placed,
        out_specs=(P("zero", "seq", None), P("zero", "seq", None), P(("seq", "zero"), None)),
        check_vma=False,
    )
```

```python
import functools

import jax
import jax.numpy as jnp
from jax import lax
from jax.experimental import pallas as pl
from jax.experimental.pallas import tpu as pltpu
from jax.sharding import PartitionSpec as P

F32 = jnp.float32
BF16 = jnp.bfloat16
HIGH = lax.Precision.HIGHEST
LANES = 128


def dot(a, b, dims, precision=None):
    return lax.dot_general(
        a, b, ((dims[:1], dims[1:]), ((), ())), precision=precision, preferred_element_type=F32
    )


def triangles(count):
    row = lax.broadcasted_iota(jnp.int32, (count, count), 0)
    col = lax.broadcasted_iota(jnp.int32, (count, count), 1)
    return row, col


def spread(values, first, per, width):
    lane = lax.broadcasted_iota(jnp.int32, (values.shape[0], LANES), 1)
    out = values[:, first : first + 1]
    for k in range(1, per):
        out = jnp.where(lane < k * width, out, values[:, first + k : first + k + 1])
    return jnp.broadcast_to(out, (values.shape[0], LANES))


def head_lanes(tile, k, width):
    lane = lax.broadcasted_iota(jnp.int32, tile.shape, 1)
    keep = (lane >= k * width) & (lane < (k + 1) * width)
    return jnp.where(keep, tile, jnp.zeros_like(tile))


def prepare(inner, state, heads, n_back, own_ref, *refs):
    back_refs, refs = refs[:n_back], refs[n_back:]
    bias_ref, alog_ref, g_ref, xbc_ref, raw_ref, dt_ref, cum_ref, fb_ref, dec_ref = refs
    width = inner // heads
    per = LANES // width
    count = own_ref.shape[0]
    main = inner + 2 * state
    raw = own_ref[:, main : main + heads]
    for ref in back_refs:
        raw = raw + ref[:, main : main + heads].astype(F32)
        raw = raw + ref[:, main + heads : main + 2 * heads].astype(F32)
    shifted = raw + bias_ref[...]
    dt = jnp.maximum(shifted, 0.0) + jnp.log1p(jnp.exp(-jnp.abs(shifted)))
    loga = -jnp.exp(alog_ref[...]) * dt
    row, col = triangles(count)
    lower = (row >= col).astype(F32)
    cum = dot(lower, loga, (1, 0), HIGH)
    raw_ref[...] = raw
    dt_ref[...] = dt
    cum_ref[...] = cum
    total = cum[count - 1 : count, :]
    tail = jnp.exp(total - cum) * dt
    grow = jnp.exp(cum)
    onehot = (
        lax.broadcasted_iota(jnp.int32, (heads, heads), 0)
        == lax.broadcasted_iota(jnp.int32, (heads, heads), 1)
    ).astype(F32)
    decays = jnp.broadcast_to(jnp.exp(total), (LANES, heads))
    dec_ref[...] = dot(onehot, decays, (1, 1), HIGH)

    def column(at):
        part = own_ref[:, at : at + LANES]
        for ref in back_refs:
            part = part + ref[:, at : at + LANES].astype(F32)
        return part.astype(BF16)

    for at in range(inner, main, LANES):
        xbc_ref[:, at : at + LANES] = column(at)
    bm = xbc_ref[:, inner : inner + state]
    cm = xbc_ref[:, inner + state : main]
    for j in range(heads // per):
        at = j * LANES
        x = column(at)
        xbc_ref[:, at : at + LANES] = x
        scaled = (spread(tail, j * per, per, width) * x.astype(F32)).astype(BF16)
        fb_ref[0, at : at + LANES, :] = dot(scaled, bm, (0, 0)).astype(BF16)
        g = g_ref[:, at : at + LANES].astype(F32)
        grown = (spread(grow, j * per, per, width) * g).astype(BF16)
        fb_ref[1, at : at + LANES, :] = dot(grown, cm, (0, 0)).astype(BF16)


def within(inner, state, heads, xbc_ref, g_ref, dt_ref, cum_ref, y_ref, v_ref, w_ref):
    width = inner // heads
    per = LANES // width
    count = dt_ref.shape[0]
    main = inner + 2 * state
    bm = xbc_ref[:, inner : inner + state]
    cm = xbc_ref[:, inner + state : main]
    dt = dt_ref[...]
    cum = cum_ref[...]
    row, col = triangles(count)
    eye = (row == col).astype(F32)
    cum_rows = dot(cum, eye, (0, 0), HIGH)
    dt_rows = dot(dt, eye, (0, 0), HIGH)
    later = row >= col
    scores = dot(cm, bm, (1, 1))
    mixed = jnp.zeros((count, count), F32)
    for j in range(heads // per):
        at = j * LANES
        x = xbc_ref[:, at : at + LANES]
        g = g_ref[:, at : at + LANES]
        xdt = (spread(dt, j * per, per, width) * x.astype(F32)).astype(BF16)
        y = jnp.zeros((count, LANES), F32)
        v = jnp.zeros((count, LANES), F32)
        for k in range(per):
            h = j * per + k
            span = jnp.where(later, cum[:, h : h + 1] - cum_rows[h : h + 1, :], -1e30)
            decay = jnp.exp(span)
            weights = (scores * decay).astype(BF16)
            gk = head_lanes(g, k, width)
            mixed = mixed + decay * dt_rows[h : h + 1, :] * dot(gk, x, (1, 1))
            y = y + dot(weights, head_lanes(xdt, k, width), (1, 0))
            v = v + dot(weights, gk, (0, 0))
        y_ref[:, at : at + LANES] = y
        v_ref[:, at : at + LANES] = v
    w_ref[...] = mixed


def across(
    inner, state, heads, xbc_ref, g_ref, raw_ref, dt_ref, cum_ref, bias_ref, alog_ref, skip_ref,
    y_ref, v_ref, w_ref, se_ref, out_ref, gp_ref
):
    width = inner // heads
    per = LANES // width
    count = dt_ref.shape[0]
    main = inner + 2 * state
    bm = xbc_ref[:, inner : inner + state]
    cm = xbc_ref[:, inner + state : main]
    dt = dt_ref[...]
    cum = cum_ref[...]
    total = cum[count - 1 : count, :]
    grow = jnp.exp(cum)
    tail = jnp.exp(total - cum)
    skip = jnp.broadcast_to(skip_ref[...], (8, heads))
    mixed = w_ref[...].astype(BF16)
    grad_b = dot(mixed, cm, (0, 0))
    grad_c = dot(mixed, bm, (1, 0))
    head = lax.broadcasted_iota(jnp.int32, (count, heads), 1)
    head8 = lax.broadcasted_iota(jnp.int32, (8, heads), 1)
    near = jnp.zeros((count, heads), F32)
    far = jnp.zeros((count, heads), F32)
    direct = jnp.zeros((count, heads), F32)
    inside = jnp.zeros((8, heads), F32)
    for j in range(heads // per):
        at = j * LANES
        x16 = xbc_ref[:, at : at + LANES]
        x = x16.astype(F32)
        g = g_ref[:, at : at + LANES].astype(F32)
        start = se_ref[0, at : at + LANES, :]
        end = se_ref[1, at : at + LANES, :]
        dts = spread(dt, j * per, per, width)
        grows = spread(grow, j * per, per, width)
        tails = spread(tail, j * per, per, width)
        skips = spread(skip, j * per, per, width)[0:1, :]
        y = y_ref[:, at : at + LANES] + grows * dot(cm, start, (1, 1))
        v_in = v_ref[:, at : at + LANES]
        v_out = tails * dot(bm, end, (1, 1))
        v = v_in + v_out
        out_ref[:, at : at + LANES] = (y + skips * x).astype(BF16)
        gp_ref[:, at : at + LANES] = (dts * v + skips * g).astype(BF16)
        xdt = dts * x
        grad_b = grad_b + dot((tails * xdt).astype(BF16), end, (1, 0))
        grad_c = grad_c + dot((grows * g).astype(BF16), start, (1, 0))
        a = g * y - xdt.astype(BF16).astype(F32) * v_in
        q = xdt * v_out
        d = x * v
        es = end.astype(F32) * start.astype(F32)
        for k in range(per):
            h = j * per + k
            near = jnp.where(head == h, jnp.sum(head_lanes(a, k, width), 1, keepdims=True), near)
            far = jnp.where(head == h, jnp.sum(head_lanes(q, k, width), 1, keepdims=True), far)
            direct = jnp.where(head == h, jnp.sum(head_lanes(d, k, width), 1, keepdims=True), direct)
            rows = jnp.sum(es[k * width : (k + 1) * width, :], axis=0, keepdims=True)
            value = jnp.sum(rows, axis=1, keepdims=True)
            inside = jnp.where(head8 == h, value, inside)
    row, col = triangles(count)
    upper = (row <= col).astype(F32)
    before = (row > col).astype(F32)
    dloga = dot(upper, near, (1, 0), HIGH) + dot(before, far, (1, 0), HIGH)
    dloga = dloga + jnp.exp(total) * inside[0:1, :]
    slope = jax.nn.sigmoid(raw_ref[...] + bias_ref[...])
    grad_raw = slope * (direct - jnp.exp(alog_ref[...]) * dloga)
    gp_ref[:, inner : inner + state] = grad_b.astype(BF16)
    gp_ref[:, inner + state : main] = grad_c.astype(BF16)
    gp_ref[:, main : main + heads] = grad_raw.astype(BF16)


def local_call(body, outs, flops, name, *args):
    size = sum(a.size * a.dtype.itemsize for a in args)
    return pl.pallas_call(
        body,
        out_shape=outs,
        in_specs=[pl.BlockSpec(memory_space=pltpu.VMEM)] * len(args),
        out_specs=jax.tree.map(lambda _: pl.BlockSpec(memory_space=pltpu.VMEM), outs),
        cost_estimate=pl.CostEstimate(flops=flops, bytes_accessed=size, transcendentals=0),
        compiler_params=pltpu.CompilerParams(vmem_limit_bytes=40 * 2**20),
        name=name,
    )(*args)


def take(parts, at):
    return lax.dynamic_index_in_dim(parts, at, 0, keepdims=False)


def shifted_pairs(total, factor, stride, by):
    pairs = []
    for i in range(total):
        at = (i // stride) % factor
        pairs.append((i, i + ((at + by) % factor - at) * stride))
    return pairs


def deal(parts, axis, factor, stride):
    total = lax.axis_size(axis)
    me = (lax.axis_index(axis) // stride) % factor
    got = [take(parts, me)]
    for by in range(1, factor):
        piece = take(parts, (me + by) % factor)
        got.append(lax.ppermute(piece, axis, shifted_pairs(total, factor, stride, by)))
    return got


def in_order(got, axis, factor, stride):
    me = (lax.axis_index(axis) // stride) % factor
    if factor == 2:
        first = me == 0
        return [jnp.where(first, got[0], got[1]), jnp.where(first, got[1], got[0])]
    stacked = jnp.stack(got)
    return [take(stacked, (me - i) % factor) for i in range(factor)]


def exchange(parts, factor, stride):
    return in_order(deal(parts, "seq", factor, stride), "seq", factor, stride)


def carried(pair, decay, levels, beside):
    (factor, stride), rest = levels[0], levels[1:]
    heads, width, state = pair.shape[1:]
    share = heads // factor
    parts = pair.reshape(2, factor, share, width, state).swapaxes(0, 1)
    got = deal(parts, "seq", factor, stride)
    if len(levels) == 2:
        got, near = lax.optimization_barrier((got, beside[0]))
        beside = (near, beside[1])
    if len(levels) == 1:
        got, theirs = lax.optimization_barrier((got, beside[1]))
        beside = (beside[0], theirs)
    got = [p.astype(F32) for p in in_order(got, "seq", factor, stride)]
    dec = exchange(decay.reshape(factor, share, LANES), factor, stride)
    mul = [d[:, None, :state] for d in dec]
    if rest:
        ahead, behind, product = got[0][0], got[-1][1], dec[0]
        for i in range(1, factor):
            ahead = mul[i] * ahead + got[i][0]
            product = product * dec[i]
        for i in range(factor - 2, -1, -1):
            behind = mul[i] * behind + got[i][1]
        node, beside = carried(jnp.stack([ahead, behind]).astype(BF16), product, rest, beside)
        node = node.astype(F32)
        start, end = node[0], node[1]
    else:
        start = end = jnp.zeros((share, width, state), F32)
    starts, ends = [start], [end]
    for i in range(factor - 1):
        starts.append(mul[i] * starts[-1] + got[i][0])
    for i in range(factor - 1, 0, -1):
        ends.append(mul[i] * ends[-1] + got[i][1])
    ends = ends[::-1]
    send = jnp.stack([jnp.stack([s, e]) for s, e in zip(starts, ends)]).astype(BF16)
    return jnp.concatenate(exchange(send, factor, stride), axis=1), beside


def ring_sum(chunk, factor, stride):
    total = lax.axis_size("seq")
    me = (lax.axis_index("seq") // stride) % factor
    if factor == 1:
        return chunk(me)
    far = factor // 2
    running = {1: None, -1: None}
    for distance in range(far, 0, -1):
        for way in (1, -1):
            if 2 * distance > factor or (way < 0 and factor == 2):
                continue
            if 2 * distance == factor and factor > 2:
                mine = chunk((me + far) % factor)
                half = mine.shape[0] // 2
                mine = mine[:half] if way > 0 else mine[half:]
            else:
                mine = chunk((me + way * distance) % factor)
            came = running[way]
            if came is not None:
                came = came.astype(F32)
                if came.shape[0] < mine.shape[0]:
                    half = came.shape[0]
                    if way > 0:
                        mine = jnp.concatenate([mine[:half] + came, mine[half:]], axis=0)
                    else:
                        mine = jnp.concatenate([mine[:half], mine[half:] + came], axis=0)
                else:
                    mine = mine + came
            running[way] = lax.ppermute(
                mine.astype(BF16), "seq", shifted_pairs(total, factor, stride, way)
            )
    out = chunk(me)
    for way in (1, -1):
        if running[way] is None:
            continue
        came = running[way].astype(F32)
        half = came.shape[0]
        if half == out.shape[0]:
            out = out + came
        elif way > 0:
            out = jnp.concatenate([out[:half] + came, out[half:]], axis=0)
        else:
            out = jnp.concatenate([out[:half], out[half:] + came], axis=0)
    return out


def reduced(left, right, outer_first, outer_stride, mid_stride):
    rows, outer, mid, piece = left.shape

    def product(cols):
        return lax.dot_general(
            cols.reshape(rows, -1), right, (((0,), (0,)), ((), ())), preferred_element_type=F32
        )

    if outer_first:
        def chunk(at):
            return product(lax.dynamic_index_in_dim(left, at, 1, keepdims=False))

        first = ring_sum(chunk, outer, outer_stride).reshape(mid, piece, -1)
        return ring_sum(lambda at: take(first, at), mid, mid_stride)

    def chunk(at):
        return product(lax.dynamic_index_in_dim(left, at, 2, keepdims=False))

    first = ring_sum(chunk, mid, mid_stride).reshape(outer, piece, -1)
    return ring_sum(lambda at: take(first, at), outer, outer_stride)


def per_device(tokens, w_in, a_log, dt_bias, d_skip, grad_y):
    count, width = tokens.shape[1:]
    inner = grad_y.shape[2]
    heads = a_log.shape[0]
    columns = w_in.shape[1]
    state = (columns - inner - heads) // 2
    main = inner + 2 * state
    seq_count = lax.axis_size("seq")
    zero_count = lax.axis_size("zero")
    depth = w_in.shape[0]
    piece = width // (seq_count * zero_count)
    core = 2 if seq_count % 2 == 0 else 1
    mid = 2 if (seq_count // core) % 2 == 0 else 1
    outer = seq_count // (core * mid)
    rows = tokens.reshape(count, width)
    g = grad_y.reshape(count, inner)
    bias = dt_bias.reshape(1, heads)
    alog = a_log.reshape(1, heads)
    skip = d_skip.reshape(1, heads)

    slices = rows.reshape(count, zero_count, depth).swapaxes(0, 1)
    mine = deal(slices, "zero", zero_count, 1)
    backs = []
    for by in range(1, zero_count):
        part = jnp.dot(mine[by], w_in, preferred_element_type=F32)
        raw = part[:, main:]
        high = lax.reduce_precision(raw, 8, 7)
        sent = jnp.concatenate(
            [part[:, :main].astype(BF16), high.astype(BF16), (raw - high).astype(BF16)], axis=1
        )
        backs.append(
            lax.ppermute(sent, "zero", shifted_pairs(zero_count, zero_count, 1, -by))
        )
    own = jnp.dot(mine[0], w_in, preferred_element_type=F32)

    small = jax.ShapeDtypeStruct((count, heads), F32)
    xbc, raw, dt, cum, pair, decay = local_call(
        functools.partial(prepare, inner, state, heads, len(backs)),
        (
            jax.ShapeDtypeStruct((count, main), BF16),
            small,
            small,
            small,
            jax.ShapeDtypeStruct((2, inner, state), BF16),
            jax.ShapeDtypeStruct((heads, LANES), F32),
        ),
        4 * count * inner * state,
        "prepare",
        own, *backs, bias, alog, g,
    )
    wide = jax.ShapeDtypeStruct((count, inner), F32)
    y_near, v_near, mixed = local_call(
        functools.partial(within, inner, state, heads),
        (wide, wide, jax.ShapeDtypeStruct((count, count), F32)),
        20 * count * inner * count,
        "within",
        xbc, g, dt, cum,
    )
    by_owner = rows.reshape(count, outer, mid, core, zero_count, piece).transpose(4, 3, 0, 1, 2, 5)
    by_owner = by_owner.reshape(zero_count, core, count, outer * mid * piece)
    theirs = deal(by_owner, "zero", zero_count, 1)
    levels = [lv for lv in ((core, 1), (mid, core), (outer, core * mid)) if lv[0] > 1]
    start_end, ((y_near, v_near, mixed), theirs) = carried(
        pair.reshape(2, heads, inner // heads, state),
        decay,
        levels,
        ((y_near, v_near, mixed), theirs),
    )
    dealt = [deal(part, "seq", core, 1) for part in theirs]
    left = jnp.concatenate([part[by] for by in range(core) for part in dealt], axis=0)
    y, gproj = local_call(
        functools.partial(across, inner, state, heads),
        (
            jax.ShapeDtypeStruct((count, inner), BF16),
            jax.ShapeDtypeStruct((count, columns), BF16),
        ),
        8 * count * inner * state,
        "across",
        xbc, g, raw, dt, cum, bias, alog, skip, y_near, v_near, mixed,
        start_end.reshape(2, inner, state),
    )

    cotangents = [gproj] + [
        lax.ppermute(gproj, "zero", shifted_pairs(zero_count, zero_count, 1, by))
        for by in range(1, zero_count)
    ]
    grads = [
        lax.dot_general(c, w_in, (((1,), (1,)), ((), ())), preferred_element_type=F32).astype(BF16)
        for c in cotangents
    ]
    blocks = [grads[0]] + [
        lax.ppermute(grads[by], "zero", shifted_pairs(zero_count, zero_count, 1, -by))
        for by in range(1, zero_count)
    ]
    mine_at = lax.axis_index("zero")
    if zero_count == 2:
        ordered = in_order(blocks, "zero", zero_count, 1)
    else:
        stacked = jnp.stack(blocks)
        ordered = [take(stacked, (i - mine_at) % zero_count) for i in range(zero_count)]
    grad_tokens = jnp.concatenate(ordered, axis=1).reshape(1, count, width)

    right = list(cotangents)
    for by in range(1, core):
        pairs = shifted_pairs(seq_count, core, 1, by)
        right += [lax.ppermute(c, "seq", pairs) for c in cotangents]
    right = jnp.concatenate(right, axis=0)
    left = left.reshape(left.shape[0], outer, mid, piece)
    split = columns // 2 // LANES * LANES
    grad = jnp.concatenate(
        [
            reduced(left, right[:, :split], True, core * mid, core),
            reduced(left, right[:, split:], False, core * mid, core),
        ],
        axis=1,
    )
    return (y.reshape(1, count, inner), grad_tokens, grad)


def solution(mesh):
    placed = (P("zero", "seq", None), P("zero", None), P(), P(), P(), P("zero", "seq", None))
    return jax.shard_map(
        per_device,
        mesh=mesh,
        in_specs=placed,
        out_specs=(P("zero", "seq", None), P("zero", "seq", None), P(("seq", "zero"), None)),
        check_vma=False,
    )
```
